256 devices in a mesh: fsdp: 32 (over z, y), model: 8 (over x, core).
Axes of the slice: x: 4, y: 4, z: 8, core: 2. Of those that a mesh axis runs over, the one named last changes fastest.
Arguments:
- x_in: bfloat16 [256, 64, 3072], P('fsdp', 'model')
- gain_attn: float32 [2, 3072], replicated
- gain_mlp: float32 [2, 3072], replicated
- rope_cos: float32 [64, 64], replicated
- rope_sin: float32 [64, 64], replicated
- w_q: bfloat16 [2, 3072, 3072], P(None, 'fsdp', 'model')
- w_k: bfloat16 [2, 3072, 1024], P(None, 'fsdp', 'model')
- w_v: bfloat16 [2, 3072, 1024], P(None, 'fsdp', 'model')
- w_o: bfloat16 [2, 3072, 3072], P(None, 'model', 'fsdp')
- w_gate: bfloat16 [2, 3072, 8192], P(None, 'fsdp', 'model')
- w_up: bfloat16 [2, 3072, 8192], P(None, 'fsdp', 'model')
- w_down: bfloat16 [2, 8192, 3072], P(None, 'model', 'fsdp')
Outputs:
- output: bfloat16 [256, 64, 3072], P('fsdp', 'model')
All inputs are finite; a program needn't handle non-finite values.
Results may differ from the reference program's by a relative error of at most 0.02.
Values are sent between devices in bfloat16 or wider.
A program may use at most 768 MiB of HBM per device.

```python
import math
import jax
import jax.numpy as jnp
from jax import lax

D_MODEL = 3072
FFN = 8192
HEADS = 24
KV_HEADS = 8
HEAD_DIM = 128
BATCH = 256
SEQ = 64
LAYERS = 2
EPS = 1e-5
ROPE_BASE = 500000.0


def rope_tables(rng_key):
    pos_steps = jax.random.randint(rng_key, (SEQ,), 1, 4)
    positions = (jnp.cumsum(pos_steps) - pos_steps[0]).astype(jnp.float32)
    inv_freq = ROPE_BASE ** (-jnp.arange(HEAD_DIM // 2, dtype=jnp.float32) * (2.0 / HEAD_DIM))
    angles = positions[:, None] * inv_freq[None, :]
    return jnp.cos(angles), jnp.sin(angles)


def setup_inputs(seed: int = 0) -> dict:
    key_list = jax.random.split(jax.random.key(seed), 12)
    q_scale = math.sqrt(max(1.0, math.log(SEQ / 16.0)))

    def normal(rng_key, arr_shape, std_scale):
        return (jax.random.normal(rng_key, arr_shape, jnp.float32) * std_scale).astype(jnp.bfloat16)

    rope_cos, rope_sin = rope_tables(key_list[3])
    return {
        'x_in': normal(key_list[0], (BATCH, SEQ, D_MODEL), 1.0),
        'gain_attn': jax.random.uniform(key_list[1], (LAYERS, D_MODEL), jnp.float32, 0.5, 1.5),
        'gain_mlp': jax.random.uniform(key_list[2], (LAYERS, D_MODEL), jnp.float32, 0.5, 1.5),
        'rope_cos': rope_cos,
        'rope_sin': rope_sin,
        'w_q': normal(key_list[4], (LAYERS, D_MODEL, HEADS * HEAD_DIM), q_scale * D_MODEL ** -0.5),
        'w_k': normal(key_list[5], (LAYERS, D_MODEL, KV_HEADS * HEAD_DIM), D_MODEL ** -0.5),
        'w_v': normal(key_list[6], (LAYERS, D_MODEL, KV_HEADS * HEAD_DIM), D_MODEL ** -0.5),
        'w_o': normal(key_list[7], (LAYERS, HEADS * HEAD_DIM, D_MODEL), 2.0 * (HEADS * HEAD_DIM) ** -0.5),
        'w_gate': normal(key_list[8], (LAYERS, D_MODEL, FFN), D_MODEL ** -0.5),
        'w_up': normal(key_list[9], (LAYERS, D_MODEL, FFN), D_MODEL ** -0.5),
        'w_down': normal(key_list[10], (LAYERS, FFN, D_MODEL), FFN ** -0.5),
    }


def rms_norm(seq_rows, gain_vec):
    rows_f = seq_rows.astype(jnp.float32)
    mean_sq = jnp.mean(rows_f * rows_f, axis=-1, keepdims=True)
    return (rows_f * lax.rsqrt(mean_sq + EPS) * gain_vec).astype(jnp.bfloat16)


def rotate(head_vals, cos_b, sin_b):
    half_dim = head_vals.shape[-1] // 2
    heads_f = head_vals.astype(jnp.float32)
    first_half = heads_f[..., :half_dim]
    second_half = heads_f[..., half_dim:]
    return jnp.concatenate([first_half * cos_b - second_half * sin_b, second_half * cos_b + first_half * sin_b], axis=-1).astype(jnp.bfloat16)


def decoder_layer(seq_rows, params, rope_cos, rope_sin):
    gain_attn, gain_mlp, w_q, w_k, w_v, w_o, w_gate, w_up, w_down = params
    group_size = HEADS // KV_HEADS
    normed = rms_norm(seq_rows, gain_attn)
    q_proj = jnp.dot(normed, w_q, preferred_element_type=jnp.float32).astype(jnp.bfloat16).reshape(SEQ, KV_HEADS, group_size, HEAD_DIM)
    k_proj = jnp.dot(normed, w_k, preferred_element_type=jnp.float32).astype(jnp.bfloat16).reshape(SEQ, KV_HEADS, HEAD_DIM)
    v_proj = jnp.dot(normed, w_v, preferred_element_type=jnp.float32).astype(jnp.bfloat16).reshape(SEQ, KV_HEADS, HEAD_DIM)
    q_rot = rotate(q_proj, rope_cos[:, None, None, :], rope_sin[:, None, None, :])
    k_rot = rotate(k_proj, rope_cos[:, None, :], rope_sin[:, None, :])
    scores = jnp.einsum('qkgd,skd->kgqs', q_rot.astype(jnp.float32), k_rot.astype(jnp.float32)) * HEAD_DIM ** -0.5
    positions = jnp.arange(SEQ)
    causal = positions[:, None] >= positions[None, :]
    scores = jnp.where(causal, scores, -jnp.inf)
    attn_probs = jax.nn.softmax(scores, axis=-1).astype(jnp.bfloat16)
    attn_out = jnp.einsum('kgqs,skd->qkgd', attn_probs.astype(jnp.float32), v_proj.astype(jnp.float32)).astype(jnp.bfloat16).reshape(SEQ, HEADS * HEAD_DIM)
    attn_sum = jnp.dot(attn_out, w_o, preferred_element_type=jnp.float32)
    mid_rows = (seq_rows.astype(jnp.float32) + attn_sum).astype(jnp.bfloat16)
    normed_mlp = rms_norm(mid_rows, gain_mlp)
    gate_acc = jnp.dot(normed_mlp, w_gate, preferred_element_type=jnp.float32)
    up_acc = jnp.dot(normed_mlp, w_up, preferred_element_type=jnp.float32)
    hidden = (jax.nn.silu(gate_acc) * up_acc).astype(jnp.bfloat16)
    mlp_sum = jnp.dot(hidden, w_down, preferred_element_type=jnp.float32)
    return (mid_rows.astype(jnp.float32) + mlp_sum).astype(jnp.bfloat16)


def reference(x_in, gain_attn, gain_mlp, rope_cos, rope_sin, w_q, w_k, w_v, w_o, w_gate, w_up, w_down):
    params = (gain_attn, gain_mlp, w_q, w_k, w_v, w_o, w_gate, w_up, w_down)

    def one_sequence(seq_rows):
        def layer_step(carry_rows, layer_params):
            return decoder_layer(carry_rows, layer_params, rope_cos, rope_sin), None
        final_rows, _ = lax.scan(layer_step, seq_rows, params)
        return final_rows

    return lax.map(one_sequence, x_in)
```

```python
import heapq

import jax
import jax.numpy as jnp
from jax import lax
from jax.experimental import pallas as pl
from jax.experimental.pallas import tpu as pltpu
from jax.sharding import PartitionSpec as P

EPS = 1e-5
MESH = pl.DeviceIdType.MESH
NZ, NY, NX = 8, 4, 4
D = 3072
HD = 128
ROWS = 96
CHUNK = 768
NCH = D // CHUNK
SCALE = HD ** -0.5
F32, BF16 = jnp.float32, jnp.bfloat16

GROUPS = (
    (0, 0, (2, 2, 2, 2)),
    (0, 1024, (3, 3, 5, 5)),
    (0, 3072, (2, 2, 2, 2)),
    (1, 0, (1, 1, 3, 3)),
    (1, 1024, (4, 4, 4, 4)),
    (1, 3072, (2, 2, 2, 2)),
)
WEIGHT = (0.0, 3.5, 3.5, 4.5, 5.5, 6.5)
OFFSET = {"A": (-7.5, 1.5), "B": (0.5, 12.5)}
DEPTH = 3
SIGN = 1
RATE, LAT = 46.0e3, 2.5


def make_slabs():
    slabs = []
    for g, (layer, first, tiles) in enumerate(GROUPS):
        col = first
        for kind, dirn, n in zip("AABB", (1, -1, 1, -1), tiles):
            slabs.append(dict(g=g, layer=layer, c0=col, n=n * 128, kind=kind, dirn=dirn))
            col += n * 128
    return slabs


def hop(slab, t):
    if slab["kind"] == "A":
        return ("y", t, 1) if t < 3 else ("z", t - 3, 4)
    return ("z", t, 1) if t < 7 else ("y", t - 7, 8)


def make_plan(slabs):
    links = [(ax, d) for ax in "yz" for d in (1, -1)]
    busy = {k: 0.0 for k in links}
    queued = {k: 0 for k in links}
    ready = {k: [] for k in links}
    plan, heap, now = [], [], 0.0

    def rank(item):
        slab, t = slabs[item[0]], item[1]
        late = 0 if t < (3 if slab["kind"] == "A" else 7) else 1
        return (WEIGHT[slab["g"]] + OFFSET[slab["kind"]][late], SIGN * t)

    def issue():
        for k in links:
            while ready[k] and queued[k] < DEPTH:
                i, t = ready[k].pop(min(range(len(ready[k])), key=lambda j: rank(ready[k][j])))
                size = hop(slabs[i], t)[2] * ROWS * slabs[i]["n"] * 2
                busy[k] = max(now, busy[k]) + size / RATE
                queued[k] += 1
                plan.append((now, "s", i, t))
                heapq.heappush(heap, (busy[k] + LAT, i, t))

    for i, slab in enumerate(slabs):
        ready[(hop(slab, 0)[0], slab["dirn"])].append((i, 0))
    issue()
    while heap:
        now, i, t = heapq.heappop(heap)
        plan.append((now, "r", i, t))
        queued[(hop(slabs[i], t)[0], slabs[i]["dirn"])] -= 1
        if t < 9:
            ready[(hop(slabs[i], t + 1)[0], slabs[i]["dirn"])].append((i, t + 1))
        issue()
    return plan


SLABS = make_slabs()
PLAN = make_plan(SLABS)


class Pump:
    def __init__(self, place, where, ssem, rsem):
        self.z, self.y, self.m = place
        self.where, self.ssem, self.rsem = where, ssem, rsem
        self.pos, self.clock = 0, 0.0
        self.last = {SLABS[i]["g"]: n for n, (_, kind, i, _) in enumerate(PLAN) if kind == "r"}
        self.left = set(range(len(SLABS)))

    def desc(self, i, t):
        slab = SLABS[i]
        d = slab["dirn"]
        axis, u, blocks = hop(slab, t)
        z, y = self.z, self.y
        ref, base = self.where(slab)
        cols = pl.ds(slab["c0"] - base, slab["n"])
        if axis == "y":
            yi = lax.rem(y - d * u + 2 * NY, NY)
            to = z * NY + lax.rem(y + d + NY, NY)
            part = ref.at[z, yi, :, cols] if blocks == 1 else ref.at[:, yi, :, cols]
        else:
            zi = lax.rem(z - d * u + 2 * NZ, NZ)
            to = lax.rem(z + d + NZ, NZ) * NY + y
            part = ref.at[zi, y, :, cols] if blocks == 1 else ref.at[zi, :, :, cols]
        return pltpu.make_async_remote_copy(
            src_ref=part, dst_ref=part, send_sem=self.ssem.at[i], recv_sem=self.rsem.at[i, t],
            device_id=(to, self.m), device_id_type=MESH)

    def step(self):
        _, kind, i, t = PLAN[self.pos]
        self.pos += 1
        if kind == "r":
            self.desc(i, t).wait_recv()
        else:
            if t > 0:
                self.desc(i, t - 1).wait_send()
            self.desc(i, t).start()

    def until(self, now):
        while self.pos < len(PLAN) and PLAN[self.pos][0] <= now:
            self.step()

    def spend(self, us):
        self.clock += us
        self.until(self.clock)

    def group(self, g):
        self.clock = max(self.clock, PLAN[self.last[g]][0])
        while self.pos <= self.last[g]:
            self.step()
        self.until(self.clock)

    def sent(self, g):
        mine = sorted(i for i in self.left if SLABS[i]["g"] == g)
        end = max(n for n, (_, _, i, _) in enumerate(PLAN) if i in mine)
        while self.pos <= end:
            self.step()
        for i in mine:
            self.desc(i, 9).wait_send()
        self.left -= set(mine)

    def finish(self):
        for g in range(len(GROUPS)):
            if any(SLABS[i]["g"] == g for i in self.left):
                self.sent(g)


def kernel(x_ref, gain_ref, cos_ref, sin_ref, wq, wk, wv, wo, wg, wu, wd,
           y_ref, wlast, w0, w1, h_all, part, cx, rx1, rx2, zbuf, res, stage,
           lsem, csem, ssem, rsem, ag_s, ag_r, rs_s, rs_r):
    f = lax.axis_index("fsdp")
    m = lax.axis_index("model")
    z, y = f // NY, lax.rem(f, NY)
    x, core = m // 2, lax.rem(m, 2)
    xp, xm, x2 = lax.rem(x + 1, NX), lax.rem(x + 3, NX), lax.rem(x + 2, NX)
    other = 1 - core
    to_p, to_m, to_c = (f, xp * 2 + core), (f, xm * 2 + core), (f, x * 2 + other)

    bar = pltpu.get_barrier_semaphore()
    partners = [to_p, to_m, to_c]
    partners += [(z * NY + lax.rem(y + d, NY), m) for d in (1, NY - 1)]
    partners += [(lax.rem(z + d, NZ) * NY + y, m) for d in (1, NZ - 1)]
    for device in partners:
        pl.semaphore_signal(bar, inc=1, device_id=device, device_id_type=MESH)
    pl.semaphore_wait(bar, len(partners))

    loads = [pltpu.make_async_copy(wd.at[1], stage, lsem.at[0])]
    n = 1
    for layer, ref in ((0, w0), (1, w1)):
        col = 0
        for src, width in ((wq, 384), (wk, 128), (wv, 128), (wo, 384), (wg, 1024), (wu, 1024), (wd, 1024)):
            if col + width <= ref.shape[-1]:
                loads.append(pltpu.make_async_copy(src.at[layer], ref.at[z, y, :, pl.ds(col, width)], lsem.at[n]))
                n += 1
            col += width
    for copy in loads:
        copy.start()
    loads[0].wait()
    out = pltpu.make_async_copy(stage, wlast.at[z, y], lsem.at[n])
    out.start()
    for copy in loads[1:]:
        copy.wait()
    out.wait()

    def where(slab):
        if slab["layer"] == 0:
            return w0, 0
        return (w1, 0) if slab["c0"] < 3072 else (wlast, 3072)

    pump = Pump((z, y, m), where, ssem, rsem)
    pump.until(0.0)

    def remote(src, dst, sems, n, device):
        return pltpu.make_async_remote_copy(
            src_ref=src, dst_ref=dst, send_sem=sems[0].at[n], recv_sem=sems[1].at[n],
            device_id=device, device_id_type=MESH)

    lo, hi = pl.ds(0, 32), pl.ds(32, 32)

    def norm(src_ref, gain_row):
        total = jnp.zeros((64, 1), F32)
        for c in range(NCH):
            v = src_ref[:, c * CHUNK:(c + 1) * CHUNK].astype(F32)
            total += jnp.sum(v * v, axis=-1, keepdims=True)
        inv = lax.rsqrt(total * (1.0 / D) + EPS)
        for c in range(NCH):
            cols = slice(c * CHUNK, (c + 1) * CHUNK)
            v = src_ref[:, cols].astype(F32)
            h_all[x, core, :, cols] = (v * inv * gain_ref[gain_row:gain_row + 1, cols]).astype(BF16)

    def gather_rows():
        sems = (ag_s, ag_r)

        def same(i, j, rows, n, device):
            return remote(h_all.at[i, j, rows], h_all.at[i, j, rows], sems, n, device)

        full = pl.ds(0, 64)
        started = [same(x, core, lo, 0, to_p), same(x, core, hi, 1, to_m), same(x, core, full, 2, to_c),
                   same(x, core, hi, 3, to_p), same(x, core, lo, 4, to_m)]
        for copy in started:
            copy.start()

        def go(copy):
            copy.start()
            started.append(copy)

        pump.spend(7.0)
        same(xm, core, lo, 0, to_p).wait_recv()
        go(same(xm, core, lo, 5, to_p))
        go(same(xm, core, lo, 7, to_c))
        same(xp, core, hi, 1, to_p).wait_recv()
        go(same(xp, core, hi, 6, to_m))
        go(same(xp, core, hi, 8, to_c))
        pump.spend(4.0)
        same(xm, core, hi, 3, to_p).wait_recv()
        go(same(xm, core, hi, 9, to_c))
        same(xp, core, lo, 4, to_p).wait_recv()
        go(same(xp, core, lo, 10, to_c))
        pump.spend(4.0)
        same(x2, core, lo, 5, to_p).wait_recv()
        go(same(x2, core, lo, 11, to_c))
        same(x2, core, hi, 6, to_p).wait_recv()
        go(same(x2, core, hi, 12, to_c))
        pump.spend(2.0)
        for i, rows, n in ((x, full, 2), (xm, lo, 7), (xp, hi, 8), (xm, hi, 9), (xp, lo, 10), (x2, lo, 11), (x2, hi, 12)):
            same(i, other, rows, n, to_p).wait_recv()
        for copy in started:
            copy.wait_send()

    def add_rows(product, src_ref, dst_ref):
        sems = (rs_s, rs_r)
        sent = []

        def go(copy):
            copy.start()
            sent.append(copy)

        def cols_of(c):
            return pl.ds(c * CHUNK, CHUNK)

        def cross(c):
            return remote(part.at[:, other, :, cols_of(c)], cx.at[:, :, cols_of(c)], sems, 7 * c, to_c)

        def first(c, side):
            n, rows, to = ((1, lo, to_p), (2, hi, to_m))[side]
            return remote(part.at[x2, core, rows, cols_of(c)], rx1.at[side, :, cols_of(c)], sems, 7 * c + n, to)

        def second(c, side, late):
            n = 3 + 2 * side + late
            rows = (hi, lo)[side ^ late]
            blk, to = ((xp, to_p), (xm, to_m))[side]
            return remote(part.at[blk, core, rows, cols_of(c)], rx2.at[side, rows, cols_of(c)], sems, 7 * c + n, to)

        def stage_b(c):
            cross(c).wait_recv()
            cols = cols_of(c)
            for i in range(NX):
                part[i, core, :, cols] = part[i, core, :, cols] + cx[i, :, cols]
            for side in (0, 1):
                go(first(c, side))
            for side in (0, 1):
                go(second(c, side, 0))

        def stage_c(c):
            cols = cols_of(c)
            for side in (0, 1):
                first(c, side).wait_recv()
                blk, rows = ((xp, lo), (xm, hi))[side]
                part[blk, core, rows, cols] = part[blk, core, rows, cols] + rx1[side, :, cols]
                go(second(c, side, 1))

        def stage_d(c):
            cols = cols_of(c)
            for side in (0, 1):
                for late in (0, 1):
                    second(c, side, late).wait_recv()
            total = part[x, core, :, cols] + rx2[0, :, cols] + rx2[1, :, cols]
            dst_ref[:, cols] = (src_ref[:, cols].astype(F32) + total).astype(BF16)

        for c in range(NCH):
            product(c)
            go(cross(c))
            if c >= 1:
                stage_b(c - 1)
            if c >= 2:
                stage_c(c - 2)
        pump.spend(2.5)
        stage_b(NCH - 1)
        pump.spend(3.0)
        stage_c(NCH - 2)
        pump.spend(5.0)
        stage_c(NCH - 1)
        for c in range(NCH):
            pump.spend(4.0)
            stage_d(c)
        for copy in sent:
            copy.wait_send()

    rows_q = lax.broadcasted_iota(jnp.int32, (64, 64), 0)
    cols_k = lax.broadcasted_iota(jnp.int32, (64, 64), 1)

    def attend(wref):
        for first, width in ((0, 256), (256, 256), (512, 128)):
            h = h_all[...].reshape(512, D)
            w = wref[:, :, :, first:first + width].reshape(D, width)
            acc = jnp.dot(h, w, preferred_element_type=F32)
            part[:, :, :, first:first + width] = acc.astype(BF16).astype(F32).reshape(4, 2, 64, width)
            pump.spend(1.2)

        def one(s, carry):
            rows = pl.ds(pl.multiple_of(s * 8, 8), 8)
            c2, n2 = cos_ref[...], sin_ref[...]

            def head(j):
                return part[:, :, rows, j * HD:(j + 1) * HD].reshape(64, HD)

            def turn(v):
                return (v * c2 + pltpu.roll(v, HD // 2, 1) * n2).astype(BF16)

            k = turn(head(3))
            v = head(4).astype(BF16)
            for j in range(3):
                q = turn(head(j))
                sc = lax.dot_general(q, k, (((1,), (1,)), ((), ())), preferred_element_type=F32) * SCALE
                sc = jnp.where(rows_q >= cols_k, sc, -jnp.inf)
                e = jnp.exp(sc - jnp.max(sc, axis=-1, keepdims=True))
                p = (e / jnp.sum(e, axis=-1, keepdims=True)).astype(BF16)
                o = jnp.dot(p, v, preferred_element_type=F32).astype(BF16)
                part[:, :, rows, j * HD:(j + 1) * HD] = o.astype(F32).reshape(4, 2, 8, HD)
            return carry

        for half in range(2):
            lax.fori_loop(half * 4, half * 4 + 4, one, 0)
            pump.spend(4.0)
        zbuf[:, 0:384] = part[:, :, :, 0:384].reshape(512, 384).astype(BF16)

    def out_product(wref, first, width, us):
        def product(c):
            def plane(i, carry):
                zi = 2 * c + i
                w = wref[zi, :, :, first:first + width].reshape(4 * ROWS, width)
                acc = lax.dot_general(zbuf[:, 0:width], w, (((1,), (1,)), ((), ())), preferred_element_type=F32)
                cols = pl.ds(pl.multiple_of(zi * 384, 128), 384)
                part[:, :, :, cols] = acc.reshape(4, 2, 64, 384)
                return carry

            lax.fori_loop(0, 2, plane, 0)
            pump.spend(us)
        return product

    def mlp_hidden(wref):
        def tile(i, carry):
            h = h_all[...].reshape(512, D)
            c0 = pl.multiple_of(1024 + i * 256, 256)
            c1 = pl.multiple_of(2048 + i * 256, 256)
            g = jnp.dot(h, wref[:, :, :, pl.ds(c0, 256)].reshape(D, 256), preferred_element_type=F32)
            u = jnp.dot(h, wref[:, :, :, pl.ds(c1, 256)].reshape(D, 256), preferred_element_type=F32)
            zbuf[:, pl.ds(pl.multiple_of(i * 256, 256), 256)] = (jax.nn.silu(g) * u).astype(BF16)
            return carry

        for half in range(2):
            lax.fori_loop(half * 2, half * 2 + 2, tile, 0)
            pump.spend(4.5)

    for layer, wref in ((0, w0), (1, w1)):
        src = x_ref if layer == 0 else res
        norm(src, layer)
        pump.spend(1.0)
        gather_rows()
        pump.group(3 * layer)
        attend(wref)
        add_rows(out_product(wref, 640, 384, 0.7), src, res)
        norm(res, 2 + layer)
        pump.spend(1.0)
        gather_rows()
        pump.group(3 * layer + 1)
        mlp_hidden(wref)
        pump.group(3 * layer + 2)
        down = out_product(w0, 3072, 1024, 1.5)
        if layer == 0:
            add_rows(down, res, res)
        else:
            pump.sent(2)
            copies = [pltpu.make_async_copy(wlast.at[2 * c:2 * c + 2], w0.at[2 * c:2 * c + 2, :, :, 3072:4096], csem.at[c])
                      for c in range(NCH)]
            for copy in copies:
                copy.start()

            def last(c):
                copies[c].wait()
                down(c)

            add_rows(last, res, y_ref)
    pump.finish()


def solution(mesh):
    act_spec = P('fsdp', 'model', None)
    col_spec = P(None, 'fsdp', 'model')
    row_spec = P(None, 'model', 'fsdp')

    def device_step(x_in, gain_attn, gain_mlp, rope_cos, rope_sin, w_q, w_k, w_v, w_o, w_gate, w_up, w_down):
        gains = jnp.concatenate([gain_attn, gain_mlp], axis=0)
        cos2 = jnp.concatenate([rope_cos, rope_cos], axis=-1)
        sin2 = jnp.concatenate([-rope_sin, rope_sin], axis=-1)
        wo_t = jnp.swapaxes(w_o, 1, 2)
        wd_t = jnp.swapaxes(w_down, 1, 2)
        vmem = pl.BlockSpec(memory_space=pltpu.VMEM)
        hbm = pl.BlockSpec(memory_space=pltpu.HBM)
        n_slabs = len(SLABS)
        out, _ = pl.pallas_call(
            kernel,
            name="layers",
            out_shape=(jax.ShapeDtypeStruct((64, D), BF16), jax.ShapeDtypeStruct((NZ, NY, ROWS, 1024), BF16)),
            in_specs=[vmem] * 4 + [hbm] * 7,
            out_specs=(vmem, hbm),
            scratch_shapes=[
                pltpu.VMEM((NZ, NY, ROWS, 4096), BF16),
                pltpu.VMEM((NZ, NY, ROWS, 3072), BF16),
                pltpu.VMEM((4, 2, 64, D), BF16),
                pltpu.VMEM((4, 2, 64, D), F32),
                pltpu.VMEM((4, 64, D), F32),
                pltpu.VMEM((2, 32, D), F32),
                pltpu.VMEM((2, 64, D), F32),
                pltpu.VMEM((512, 1024), BF16),
                pltpu.VMEM((64, D), BF16),
                pltpu.VMEM((ROWS, 1024), BF16),
                pltpu.SemaphoreType.DMA((16,)),
                pltpu.SemaphoreType.DMA((NCH,)),
                pltpu.SemaphoreType.DMA((n_slabs,)),
                pltpu.SemaphoreType.DMA((n_slabs, 10)),
                pltpu.SemaphoreType.DMA((13,)),
                pltpu.SemaphoreType.DMA((13,)),
                pltpu.SemaphoreType.DMA((7 * NCH,)),
                pltpu.SemaphoreType.DMA((7 * NCH,)),
            ],
            compiler_params=pltpu.CompilerParams(
                collective_id=0, has_side_effects=True, vmem_limit_bytes=67043328),
        )(x_in.reshape(64, D), gains, cos2, sin2, w_q, w_k, w_v, wo_t, w_gate, w_up, wd_t)
        return out.reshape(x_in.shape)

    return jax.shard_map(device_step, mesh=mesh, in_specs=(act_spec, P(), P(), P(), P(), col_spec, col_spec, col_spec, row_spec, col_spec, col_spec, row_spec), out_specs=act_spec, check_vma=False)
```

```python
import heapq

import jax
import jax.numpy as jnp
from jax import lax
from jax.experimental import pallas as pl
from jax.experimental.pallas import tpu as pltpu
from jax.sharding import PartitionSpec as P

EPS = 1e-5
MESH = pl.DeviceIdType.MESH
NZ, NY, NX = 8, 4, 4
D = 3072
HD = 128
ROWS = 96
CHUNK = 768
NCH = D // CHUNK
SCALE = HD ** -0.5
F32, BF16 = jnp.float32, jnp.bfloat16

GROUPS = (
    (0, 0, (2, 2, 2, 2)),
    (0, 1024, (2, 2, 6, 6)),
    (0, 3072, (2, 2, 2, 2)),
    (1, 0, (2, 2, 2, 2)),
    (1, 1024, (3, 3, 5, 5)),
    (1, 3072, (2, 2, 2, 2)),
)
WEIGHT = (-28.5, -23, -23, -6, 30, 30)
OFFSET = {"A": (-32, 4.5), "B": (-46, 44.5)}
SIGN = 1
AHEAD, MARGIN = 3.0, 4.0
RATE, LAT = 46.3e3, 2.2
ATTEND_US = 3.0
SEND_US, RECEIVE_US = 0.06, 0.04


def make_slabs(groups):
    slabs = []
    for g, (layer, first, tiles) in enumerate(groups):
        col = first
        for kind, dirn, n in zip("AABB", (1, -1, 1, -1), tiles):
            if n:
                slabs.append(dict(g=g, layer=layer, c0=col, n=n * 128, kind=kind, dirn=dirn))
            col += n * 128
    return slabs


def hop(slab, t):
    if slab["kind"] == "A":
        return ("y", t, 1) if t < 3 else ("z", t - 3, 4)
    return ("z", t, 1) if t < 7 else ("y", t - 7, 8)


class Planner:
    def __init__(self, slabs, weight, offset, sign, ahead, margin):
        self.slabs, self.weight, self.offset, self.sign, self.ahead, self.margin = slabs, weight, offset, sign, ahead, margin
        self.spent = 0.0
        self.links = [(ax, d) for ax in "yz" for d in (1, -1)]
        self.busy = {k: 0.0 for k in self.links}
        self.ready = {k: [] for k in self.links}
        self.heap, self.clock = [], 0.0
        self.due = {}
        self.ends = {}
        for i, slab in enumerate(slabs):
            self.ready[(hop(slab, 0)[0], slab["dirn"])].append((i, 0))
            self.due[slab["g"]] = self.due.get(slab["g"], 0) + 10

    def rank(self, item):
        slab, t = self.slabs[item[0]], item[1]
        late = 0 if t < (3 if slab["kind"] == "A" else 7) else 1
        return (self.weight[slab["g"]] + self.offset[slab["kind"]][late], self.sign * t, item)

    def send(self, i, t):
        pass

    def receive(self, i, t):
        pass

    def turn(self):
        while self.heap and self.heap[0][0] <= self.clock:
            _, i, t = heapq.heappop(self.heap)
            self.receive(i, t)
            self.spent += RECEIVE_US
            g = self.slabs[i]["g"]
            self.due[g] -= 1
            self.ends[g] = self.clock
            if t < 9:
                self.ready[(hop(self.slabs[i], t + 1)[0], self.slabs[i]["dirn"])].append((i, t + 1))
        self.issue(self.ahead)

    def issue(self, ahead):
        for k in self.links:
            while self.ready[k] and self.busy[k] - self.clock < ahead:
                item = min(self.ready[k], key=self.rank)
                self.ready[k].remove(item)
                i, t = item
                size = hop(self.slabs[i], t)[2] * ROWS * self.slabs[i]["n"] * 2
                self.busy[k] = max(self.clock, self.busy[k]) + size / RATE
                self.send(i, t)
                self.spent += SEND_US
                heapq.heappush(self.heap, (self.busy[k] + LAT, i, t))

    def fill(self, us):
        self.spent = 0.0
        self.issue(us + self.margin)
        self.clock += self.spent

    def work(self, us):
        self.clock += us
        self.spent = 0.0
        self.turn()
        self.clock += self.spent

    def idle(self, us):
        end = self.clock + us
        while self.heap and self.heap[0][0] <= end:
            self.clock = max(self.clock, self.heap[0][0])
            self.turn()
        self.clock = end

    def group(self, g):
        while self.due[g]:
            self.clock = max(self.clock, self.heap[0][0])
            self.turn()


SLABS = make_slabs(GROUPS)


class Pump(Planner):
    def __init__(self, place, where, before, spare, ssem, rsem):
        super().__init__(SLABS, WEIGHT, OFFSET, SIGN, AHEAD, MARGIN)
        z, y, self.m = place
        self.z, self.y = z, y
        self.where, self.before, self.spare, self.ssem, self.rsem = where, before, spare, ssem, rsem
        self.left = set(range(len(SLABS)))
        self.zs = [z] + [lax.rem(z + u, NZ) for u in range(1, NZ)]
        self.ys = [y] + [lax.rem(y + u, NY) for u in range(1, NY)]
        self.to = {("y", d): z * NY + self.ys[d % NY] for d in (1, -1)}
        self.to.update({("z", d): self.zs[d % NZ] * NY + y for d in (1, -1)})

    def desc(self, i, t):
        slab = SLABS[i]
        d = slab["dirn"]
        axis, u, blocks = hop(slab, t)
        ref, base = self.where(slab)
        cols = pl.ds(slab["c0"] - base, slab["n"])
        if axis == "y":
            yi = self.ys[-d * u % NY]
            part = ref.at[self.z, yi, :, cols] if blocks == 1 else ref.at[:, yi, :, cols]
        else:
            zi = self.zs[-d * u % NZ]
            part = ref.at[zi, self.y, :, cols] if blocks == 1 else ref.at[zi, :, :, cols]
        return pltpu.make_async_remote_copy(
            src_ref=part, dst_ref=part, send_sem=self.ssem.at[i], recv_sem=self.rsem.at[i, t],
            device_id=(self.to[axis, d], self.m), device_id_type=MESH)

    def send(self, i, t):
        if t == 0:
            self.before(SLABS[i])
        self.desc(i, t).start()

    def receive(self, i, t):
        self.desc(i, t).wait_recv()

    def sent(self, g):
        self.group(g)
        for i in sorted(i for i in self.left if SLABS[i]["g"] == g):
            whole = self.spare.at[pl.ds(0, NZ * NY - 1), :, pl.ds(0, SLABS[i]["n"])]
            pltpu.make_async_copy(whole, whole, self.ssem.at[i]).wait()
            self.left.remove(i)

    def finish(self):
        for g in range(len(GROUPS)):
            self.sent(g)


def kernel(x_ref, gain_a, gain_m, cos_ref, sin_ref, wq, wk, wv, wo, wg, wu, wd,
           y_ref, wlast, w0, w1, h_all, part, cx, rx1, rx2, zbuf, res, stage, cos2, sin2,
           lsem, csem, ssem, rsem, ag_s, ag_r, rs_s, rs_r):
    f = lax.axis_index("fsdp")
    m = lax.axis_index("model")
    z, y = f // NY, lax.rem(f, NY)
    x, core = m // 2, lax.rem(m, 2)
    xp, xm, x2 = lax.rem(x + 1, NX), lax.rem(x + 3, NX), lax.rem(x + 2, NX)
    other = 1 - core
    to_p, to_m, to_c = (f, xp * 2 + core), (f, xm * 2 + core), (f, x * 2 + other)

    loads = []
    for layer, ref in ((0, w0), (1, w1)):
        col = 0
        for src, width in ((wq, 384), (wk, 128), (wv, 128), (wo, 384), (wg, 1024), (wu, 1024), (wd, 1024)):
            to = ref.at[z, y, :, pl.ds(col, width)] if col + width <= ref.shape[-1] else stage
            copy = pltpu.make_async_copy(src.at[layer], to, lsem.at[len(loads)])
            copy.start()
            loads.append((layer, col, width, copy))
            col += width
    waited = set()

    def before(slab):
        for n, (layer, col, width, copy) in enumerate(loads):
            if layer == slab["layer"] and col < slab["c0"] + slab["n"] and slab["c0"] < col + width and n not in waited:
                waited.add(n)
                if n < len(loads) - 1:
                    copy.wait()

    bar = pltpu.get_barrier_semaphore()
    partners = [to_p, to_m, to_c]
    partners += [(z * NY + lax.rem(y + d, NY), m) for d in (1, NY - 1)]
    partners += [(lax.rem(z + d, NZ) * NY + y, m) for d in (1, NZ - 1)]
    for device in partners:
        pl.semaphore_signal(bar, inc=1, device_id=device, device_id_type=MESH)

    def norm(src_ref, gain_ref, layer):
        total = jnp.zeros((64, 1), F32)
        for c in range(NCH):
            v = src_ref[:, c * CHUNK:(c + 1) * CHUNK].astype(F32)
            total += jnp.sum(v * v, axis=-1, keepdims=True)
        inv = lax.rsqrt(total * (1.0 / D) + EPS)
        for c in range(NCH):
            cols = slice(c * CHUNK, (c + 1) * CHUNK)
            v = src_ref[:, cols].astype(F32)
            h_all[x, core, :, cols] = (v * inv * gain_ref[layer:layer + 1, cols]).astype(BF16)

    norm(x_ref, gain_a, 0)
    cos2[...] = jnp.concatenate([cos_ref[...], cos_ref[...]], axis=-1)
    sin2[...] = jnp.concatenate([-sin_ref[...], sin_ref[...]], axis=-1)

    loads[-1][3].wait()
    out = pltpu.make_async_copy(stage, wlast.at[z, y], lsem.at[len(loads)])
    out.start()
    pl.semaphore_wait(bar, len(partners))
    out.wait()

    def where(slab):
        if slab["layer"] == 0:
            return w0, 0
        return (w1, 0) if slab["c0"] < 3072 else (wlast, 3072)

    pump = Pump((z, y, m), where, before, wlast.reshape(NZ * NY, ROWS, 1024), ssem, rsem)

    def remote(src, dst, sems, n, device):
        return pltpu.make_async_remote_copy(
            src_ref=src, dst_ref=dst, send_sem=sems[0].at[n], recv_sem=sems[1].at[n],
            device_id=device, device_id_type=MESH)

    lo, hi = pl.ds(0, 32), pl.ds(32, 32)
    leaving = []

    def settle():
        for copy in leaving:
            copy.wait_send()
        leaving.clear()

    def gather_rows():
        sems = (ag_s, ag_r)

        def same(i, j, rows, n, device):
            return remote(h_all.at[i, j, rows], h_all.at[i, j, rows], sems, n, device)

        full = pl.ds(0, 64)
        started = [same(x, core, lo, 0, to_p), same(x, core, hi, 1, to_m), same(x, core, full, 2, to_c),
                   same(x, core, hi, 3, to_p), same(x, core, lo, 4, to_m)]
        for copy in started:
            copy.start()
        pump.turn()
        settle()

        def go(copy):
            copy.start()
            started.append(copy)

        pump.idle(7.0)
        same(xm, core, lo, 0, to_p).wait_recv()
        go(same(xm, core, lo, 5, to_p))
        go(same(xm, core, lo, 7, to_c))
        same(xp, core, hi, 1, to_p).wait_recv()
        go(same(xp, core, hi, 6, to_m))
        go(same(xp, core, hi, 8, to_c))
        pump.idle(4.0)
        same(xm, core, hi, 3, to_p).wait_recv()
        go(same(xm, core, hi, 9, to_c))
        same(xp, core, lo, 4, to_p).wait_recv()
        go(same(xp, core, lo, 10, to_c))
        pump.idle(4.0)
        same(x2, core, lo, 5, to_p).wait_recv()
        go(same(x2, core, lo, 11, to_c))
        same(x2, core, hi, 6, to_p).wait_recv()
        go(same(x2, core, hi, 12, to_c))
        pump.idle(2.0)
        for i, rows, n in ((x, full, 2), (xm, lo, 7), (xp, hi, 8), (xm, hi, 9), (xp, lo, 10), (x2, lo, 11), (x2, hi, 12)):
            same(i, other, rows, n, to_p).wait_recv()
        leaving.extend(started)

    def add_rows(product, src_ref, dst_ref):
        sems = (rs_s, rs_r)
        sent = []

        def go(copy):
            copy.start()
            sent.append(copy)

        def cols_of(c):
            return pl.ds(c * CHUNK, CHUNK)

        def cross(c):
            return remote(part.at[:, other, :, cols_of(c)], cx.at[:, :, cols_of(c)], sems, 7 * c, to_c)

        def first(c, side):
            n, rows, to = ((1, lo, to_p), (2, hi, to_m))[side]
            return remote(part.at[x2, core, rows, cols_of(c)], rx1.at[side, :, cols_of(c)], sems, 7 * c + n, to)

        def second(c, side, late):
            n = 3 + 2 * side + late
            rows = (hi, lo)[side ^ late]
            blk, to = ((xp, to_p), (xm, to_m))[side]
            return remote(part.at[blk, core, rows, cols_of(c)], rx2.at[side, rows, cols_of(c)], sems, 7 * c + n, to)

        def stage_b(c):
            cross(c).wait_recv()
            cols = cols_of(c)
            for i in range(NX):
                part[i, core, :, cols] = part[i, core, :, cols] + cx[i, :, cols]
            for side in (0, 1):
                go(first(c, side))
            for side in (0, 1):
                go(second(c, side, 0))

        def stage_c(c):
            cols = cols_of(c)
            for side in (0, 1):
                first(c, side).wait_recv()
                blk, rows = ((xp, lo), (xm, hi))[side]
                part[blk, core, rows, cols] = part[blk, core, rows, cols] + rx1[side, :, cols]
                go(second(c, side, 1))

        def stage_d(c):
            cols = cols_of(c)
            for side in (0, 1):
                for late in (0, 1):
                    second(c, side, late).wait_recv()
            total = part[x, core, :, cols] + rx2[0, :, cols] + rx2[1, :, cols]
            dst_ref[:, cols] = (src_ref[:, cols].astype(F32) + total).astype(BF16)

        for c in range(NCH):
            product(c)
            go(cross(c))
            if c >= 1:
                stage_b(c - 1)
            if c >= 2:
                stage_c(c - 2)
        pump.idle(1.0)
        settle()
        pump.idle(1.0)
        stage_b(NCH - 1)
        pump.idle(3.0)
        stage_c(NCH - 2)
        pump.idle(5.0)
        stage_c(NCH - 1)
        for c in range(NCH):
            pump.idle((0.5, 4.0, 6.0, 6.0)[c])
            stage_d(c)
        leaving.extend(sent)

    rows_q = lax.broadcasted_iota(jnp.int32, (64, 64), 0)
    cols_k = lax.broadcasted_iota(jnp.int32, (64, 64), 1)
    one_head = (rows_q >= cols_k).astype(F32)
    seen = jnp.concatenate([one_head] * 3, axis=0) > 0.5

    def attend(wref):
        for first, width in ((0, 256), (256, 256), (512, 128)):
            pump.fill(1.2)
            h = h_all[...].reshape(512, D)
            w = wref[:, :, :, first:first + width].reshape(D, width)
            acc = jnp.dot(h, w, preferred_element_type=F32)
            part[:, :, :, first:first + width] = acc.astype(BF16).astype(F32).reshape(4, 2, 64, width)
            pump.work(1.2)

        def pair(i, carry):
            c2, n2 = cos2[...], sin2[...]
            c3, n3 = jnp.concatenate([c2] * 3, axis=0), jnp.concatenate([n2] * 3, axis=0)

            def turn(v, c, n):
                return (v * c + pltpu.roll(v, HD // 2, 1) * n).astype(BF16)

            both = []
            for j in range(2):
                rows = pl.ds(pl.multiple_of(i * 16 + j * 8, 8), 8)
                heads = [part[:, :, rows, h * HD:(h + 1) * HD].reshape(64, HD) for h in range(5)]
                both.append((rows, jnp.concatenate(heads[:3], axis=0), heads[3], heads[4]))
            outs = []
            for rows, q, k, v in both:
                sc = lax.dot_general(turn(q, c3, n3), turn(k, c2, n2), (((1,), (1,)), ((), ())),
                                     preferred_element_type=F32) * SCALE
                sc = jnp.where(seen, sc, -jnp.inf)
                e = jnp.exp(sc - jnp.max(sc, axis=-1, keepdims=True))
                p = (e / jnp.sum(e, axis=-1, keepdims=True)).astype(BF16)
                outs.append(jnp.dot(p, v.astype(BF16), preferred_element_type=F32).astype(BF16).astype(F32))
            for (rows, _, _, _), o in zip(both, outs):
                for h in range(3):
                    part[:, :, rows, h * HD:(h + 1) * HD] = o[h * 64:(h + 1) * 64].reshape(4, 2, 8, HD)
            return carry

        for half in range(2):
            pump.fill(ATTEND_US)
            lax.fori_loop(half * 2, half * 2 + 2, pair, 0)
            pump.work(ATTEND_US)
        zbuf[:, 0:384] = part[:, :, :, 0:384].reshape(512, 384).astype(BF16)

    def out_product(wref, first, width, us):
        def product(c):
            def plane(i, carry):
                zi = 2 * c + i
                w = wref[zi, :, :, first:first + width].reshape(4 * ROWS, width)
                acc = lax.dot_general(zbuf[:, 0:width], w, (((1,), (1,)), ((), ())), preferred_element_type=F32)
                cols = pl.ds(pl.multiple_of(zi * 384, 128), 384)
                part[:, :, :, cols] = acc.reshape(4, 2, 64, 384)
                return carry

            pump.fill(us)
            lax.fori_loop(0, 2, plane, 0)
            pump.work(us)
        return product

    def mlp_hidden(wref):
        def tile(i, carry):
            h = h_all[...].reshape(512, D)
            c0 = pl.multiple_of(1024 + i * 256, 256)
            c1 = pl.multiple_of(2048 + i * 256, 256)
            g = jnp.dot(h, wref[:, :, :, pl.ds(c0, 256)].reshape(D, 256), preferred_element_type=F32)
            u = jnp.dot(h, wref[:, :, :, pl.ds(c1, 256)].reshape(D, 256), preferred_element_type=F32)
            zbuf[:, pl.ds(pl.multiple_of(i * 256, 256), 256)] = (jax.nn.silu(g) * u).astype(BF16)
            return carry

        for half in range(2):
            pump.fill(3.7)
            lax.fori_loop(half * 2, half * 2 + 2, tile, 0)
            pump.work(3.7)

    for layer, wref in ((0, w0), (1, w1)):
        src = x_ref if layer == 0 else res
        if layer:
            norm(src, gain_a, layer)
            pump.work(1.0)
        gather_rows()
        pump.group(3 * layer)
        attend(wref)
        add_rows(out_product(wref, 640, 384, 0.7), src, res)
        norm(res, gain_m, layer)
        pump.work(1.0)
        gather_rows()
        pump.group(3 * layer + 1)
        mlp_hidden(wref)
        pump.group(3 * layer + 2)
        down = out_product(w0, 3072, 1024, 1.5)
        if layer == 0:
            add_rows(down, res, res)
        else:
            pump.sent(2)
            copies = [pltpu.make_async_copy(wlast.at[2 * c:2 * c + 2], w0.at[2 * c:2 * c + 2, :, :, 3072:4096], csem.at[c])
                      for c in range(NCH)]
            for copy in copies:
                copy.start()

            def last(c):
                copies[c].wait()
                down(c)

            add_rows(last, res, y_ref)
    settle()
    pump.finish()


def solution(mesh):
    act_spec = P('fsdp', 'model', None)
    col_spec = P(None, 'fsdp', 'model')
    row_spec = P(None, 'model', 'fsdp')

    def device_step(x_in, gain_attn, gain_mlp, rope_cos, rope_sin, w_q, w_k, w_v, w_o, w_gate, w_up, w_down):
        wo_t = jnp.swapaxes(w_o, 1, 2)
        wd_t = jnp.swapaxes(w_down, 1, 2)
        vmem = pl.BlockSpec(memory_space=pltpu.VMEM)
        hbm = pl.BlockSpec(memory_space=pltpu.HBM)
        n_slabs = len(SLABS)
        out, _ = pl.pallas_call(
            kernel,
            name="layers",
            out_shape=(jax.ShapeDtypeStruct((64, D), BF16), jax.ShapeDtypeStruct((NZ, NY, ROWS, 1024), BF16)),
            in_specs=[vmem] * 5 + [hbm] * 7,
            out_specs=(vmem, hbm),
            scratch_shapes=[
                pltpu.VMEM((NZ, NY, ROWS, 4096), BF16),
                pltpu.VMEM((NZ, NY, ROWS, 3072), BF16),
                pltpu.VMEM((4, 2, 64, D), BF16),
                pltpu.VMEM((4, 2, 64, D), F32),
                pltpu.VMEM((4, 64, D), F32),
                pltpu.VMEM((2, 32, D), F32),
                pltpu.VMEM((2, 64, D), F32),
                pltpu.VMEM((512, 1024), BF16),
                pltpu.VMEM((64, D), BF16),
                pltpu.VMEM((ROWS, 1024), BF16),
                pltpu.VMEM((64, HD), F32),
                pltpu.VMEM((64, HD), F32),
                pltpu.SemaphoreType.DMA((16,)),
                pltpu.SemaphoreType.DMA((NCH,)),
                pltpu.SemaphoreType.DMA((n_slabs,)),
                pltpu.SemaphoreType.DMA((n_slabs, 10)),
                pltpu.SemaphoreType.DMA((13,)),
                pltpu.SemaphoreType.DMA((13,)),
                pltpu.SemaphoreType.DMA((7 * NCH,)),
                pltpu.SemaphoreType.DMA((7 * NCH,)),
            ],
            compiler_params=pltpu.CompilerParams(
                collective_id=0, has_side_effects=True, vmem_limit_bytes=67043328),
        )(x_in.reshape(64, D), gain_attn, gain_mlp, rope_cos, rope_sin, w_q, w_k, w_v, wo_t, w_gate, w_up, wd_t)
        return out.reshape(x_in.shape)

    return jax.shard_map(device_step, mesh=mesh, in_specs=(act_spec, P(), P(), P(), P(), col_spec, col_spec, col_spec, row_spec, col_spec, col_spec, row_spec), out_specs=act_spec, check_vma=False)
```

```python
import heapq

import jax
import jax.numpy as jnp
from jax import lax
from jax.experimental import pallas as pl
from jax.experimental.pallas import tpu as pltpu
from jax.sharding import PartitionSpec as P

EPS = 1e-5
MESH = pl.DeviceIdType.MESH
NZ, NY, NX = 8, 4, 4
D = 3072
HD = 128
ROWS = 96
CHUNK = 768
NCH = D // CHUNK
SCALE = HD ** -0.5
F32, BF16 = jnp.float32, jnp.bfloat16

GROUPS = (
    (0, 0, (2, 2, 2, 2)),
    (0, 1024, (2, 2, 6, 6)),
    (0, 3072, (2, 2, 2, 2)),
    (1, 0, (2, 2, 2, 2)),
    (1, 1024, (4, 4, 4, 4)),
    (1, 3072, (1, 1, 3, 3)),
)
WEIGHT = (-19.0, -13.5, -8.5, 13.5, 15.0, 43.0)
OFFSET = {"A": (-39.5, -6.5), "B": (-48.0, 49.0)}
SIGN = 1
AHEAD, MARGIN = 3.0, 4.0
ATTEND_US = 2.3
RATE, LAT = 46.3e3, 2.2
SEND_US, RECEIVE_US = 0.06, 0.04


def make_slabs(groups):
    slabs = []
    for g, (layer, first, tiles) in enumerate(groups):
        col = first
        for kind, dirn, n in zip("AABB", (1, -1, 1, -1), tiles):
            if n:
                slabs.append(dict(g=g, layer=layer, c0=col, n=n * 128, kind=kind, dirn=dirn))
            col += n * 128
    return slabs


def hop(slab, t):
    if slab["kind"] == "A":
        return ("y", t, 1) if t < 3 else ("z", t - 3, 4)
    return ("z", t, 1) if t < 7 else ("y", t - 7, 8)


class Planner:
    def __init__(self, slabs, weight, offset, sign, ahead, margin):
        self.slabs, self.weight, self.offset, self.sign, self.ahead, self.margin = slabs, weight, offset, sign, ahead, margin
        self.spent = 0.0
        self.links = [(ax, d) for ax in "yz" for d in (1, -1)]
        self.busy = {k: 0.0 for k in self.links}
        self.ready = {k: [] for k in self.links}
        self.heap, self.clock = [], 0.0
        self.due = {}
        self.ends = {}
        for i, slab in enumerate(slabs):
            self.ready[(hop(slab, 0)[0], slab["dirn"])].append((i, 0))
            self.due[slab["g"]] = self.due.get(slab["g"], 0) + 10

    def rank(self, item):
        slab, t = self.slabs[item[0]], item[1]
        late = 0 if t < (3 if slab["kind"] == "A" else 7) else 1
        return (self.weight[slab["g"]] + self.offset[slab["kind"]][late], self.sign * t, item)

    def send(self, i, t):
        pass

    def receive(self, i, t):
        pass

    def turn(self):
        while self.heap and self.heap[0][0] <= self.clock:
            _, i, t = heapq.heappop(self.heap)
            self.receive(i, t)
            self.spent += RECEIVE_US
            g = self.slabs[i]["g"]
            self.due[g] -= 1
            self.ends[g] = self.clock
            if t < 9:
                self.ready[(hop(self.slabs[i], t + 1)[0], self.slabs[i]["dirn"])].append((i, t + 1))
        self.issue(self.ahead)

    def issue(self, ahead):
        for k in self.links:
            while self.ready[k] and self.busy[k] - self.clock < ahead:
                item = min(self.ready[k], key=self.rank)
                self.ready[k].remove(item)
                i, t = item
                size = hop(self.slabs[i], t)[2] * ROWS * self.slabs[i]["n"] * 2
                self.busy[k] = max(self.clock, self.busy[k]) + size / RATE
                self.send(i, t)
                self.spent += SEND_US
                heapq.heappush(self.heap, (self.busy[k] + LAT, i, t))

    def fill(self, us):
        self.spent = 0.0
        self.issue(us + self.margin)
        self.clock += self.spent

    def work(self, us):
        self.clock += us
        self.spent = 0.0
        self.turn()
        self.clock += self.spent

    def idle(self, us):
        end = self.clock + us
        while self.heap and self.heap[0][0] <= end:
            self.clock = max(self.clock, self.heap[0][0])
            self.turn()
        self.clock = end

    def group(self, g):
        while self.due[g]:
            self.clock = max(self.clock, self.heap[0][0])
            self.turn()


SLABS = make_slabs(GROUPS)


class Pump(Planner):
    def __init__(self, place, where, before, spare, ssem, rsem):
        super().__init__(SLABS, WEIGHT, OFFSET, SIGN, AHEAD, MARGIN)
        z, y, self.m = place
        self.z, self.y = z, y
        self.where, self.before, self.spare, self.ssem, self.rsem = where, before, spare, ssem, rsem
        self.left = set(range(len(SLABS)))
        self.zs = [z] + [lax.rem(z + u, NZ) for u in range(1, NZ)]
        self.ys = [y] + [lax.rem(y + u, NY) for u in range(1, NY)]
        self.to = {("y", d): z * NY + self.ys[d % NY] for d in (1, -1)}
        self.to.update({("z", d): self.zs[d % NZ] * NY + y for d in (1, -1)})

    def desc(self, i, t):
        slab = SLABS[i]
        d = slab["dirn"]
        axis, u, blocks = hop(slab, t)
        ref, base = self.where(slab)
        cols = pl.ds(slab["c0"] - base, slab["n"])
        if axis == "y":
            yi = self.ys[-d * u % NY]
            part = ref.at[self.z, yi, :, cols] if blocks == 1 else ref.at[:, yi, :, cols]
        else:
            zi = self.zs[-d * u % NZ]
            part = ref.at[zi, self.y, :, cols] if blocks == 1 else ref.at[zi, :, :, cols]
        return pltpu.make_async_remote_copy(
            src_ref=part, dst_ref=part, send_sem=self.ssem.at[i], recv_sem=self.rsem.at[i, t],
            device_id=(self.to[axis, d], self.m), device_id_type=MESH)

    def send(self, i, t):
        if t == 0:
            self.before(SLABS[i])
        self.desc(i, t).start()

    def receive(self, i, t):
        self.desc(i, t).wait_recv()

    def sent(self, g):
        self.group(g)
        for i in sorted(i for i in self.left if SLABS[i]["g"] == g):
            whole = self.spare.at[pl.ds(0, NZ * NY - 1), :, pl.ds(0, SLABS[i]["n"])]
            pltpu.make_async_copy(whole, whole, self.ssem.at[i]).wait()
            self.left.remove(i)

    def finish(self):
        for g in range(len(GROUPS)):
            self.sent(g)


def kernel(x_ref, gain_a, gain_m, cos_ref, sin_ref, wq, wk, wv, wo, wg, wu, wd,
           y_ref, wlast, w0, w1, h_all, part, cx, rx1, rx2, zbuf, res, stage, cos2, sin2,
           lsem, csem, ssem, rsem, ag_s, ag_r, rs_s, rs_r):
    f = lax.axis_index("fsdp")
    m = lax.axis_index("model")
    z, y = f // NY, lax.rem(f, NY)
    x, core = m // 2, lax.rem(m, 2)
    xp, xm, x2 = lax.rem(x + 1, NX), lax.rem(x + 3, NX), lax.rem(x + 2, NX)
    other = 1 - core
    to_p, to_m, to_c = (f, xp * 2 + core), (f, xm * 2 + core), (f, x * 2 + other)

    loads = []
    for layer, ref in ((0, w0), (1, w1)):
        col = 0
        for src, width in ((wq, 384), (wk, 128), (wv, 128), (wo, 384), (wg, 1024), (wu, 1024), (wd, 1024)):
            to = ref.at[z, y, :, pl.ds(col, width)] if col + width <= ref.shape[-1] else stage
            copy = pltpu.make_async_copy(src.at[layer], to, lsem.at[len(loads)])
            copy.start()
            loads.append((layer, col, width, copy))
            col += width
    waited = set()

    def before(slab):
        for n, (layer, col, width, copy) in enumerate(loads):
            if layer == slab["layer"] and col < slab["c0"] + slab["n"] and slab["c0"] < col + width and n not in waited:
                waited.add(n)
                if n < len(loads) - 1:
                    copy.wait()

    bar = pltpu.get_barrier_semaphore()
    partners = [to_p, to_m, to_c]
    partners += [(z * NY + lax.rem(y + d, NY), m) for d in (1, NY - 1)]
    partners += [(lax.rem(z + d, NZ) * NY + y, m) for d in (1, NZ - 1)]
    for device in partners:
        pl.semaphore_signal(bar, inc=1, device_id=device, device_id_type=MESH)

    def norm(src_ref, gain_ref, layer):
        total = jnp.zeros((64, 1), F32)
        for c in range(NCH):
            v = src_ref[:, c * CHUNK:(c + 1) * CHUNK].astype(F32)
            total += jnp.sum(v * v, axis=-1, keepdims=True)
        inv = lax.rsqrt(total * (1.0 / D) + EPS)
        for c in range(NCH):
            cols = slice(c * CHUNK, (c + 1) * CHUNK)
            v = src_ref[:, cols].astype(F32)
            h_all[x, core, :, cols] = (v * inv * gain_ref[layer:layer + 1, cols]).astype(BF16)

    norm(x_ref, gain_a, 0)
    cos2[...] = jnp.concatenate([cos_ref[...], cos_ref[...]], axis=-1)
    sin2[...] = jnp.concatenate([-sin_ref[...], sin_ref[...]], axis=-1)

    loads[-1][3].wait()
    out = pltpu.make_async_copy(stage, wlast.at[z, y], lsem.at[len(loads)])
    out.start()
    pl.semaphore_wait(bar, len(partners))
    out.wait()

    def where(slab):
        if slab["layer"] == 0:
            return w0, 0
        return (w1, 0) if slab["c0"] < 3072 else (wlast, 3072)

    pump = Pump((z, y, m), where, before, wlast.reshape(NZ * NY, ROWS, 1024), ssem, rsem)

    def remote(src, dst, sems, n, device):
        return pltpu.make_async_remote_copy(
            src_ref=src, dst_ref=dst, send_sem=sems[0].at[n], recv_sem=sems[1].at[n],
            device_id=device, device_id_type=MESH)

    lo, hi = pl.ds(0, 32), pl.ds(32, 32)
    leaving = []

    def settle():
        for copy in leaving:
            copy.wait_send()
        leaving.clear()

    def gather_rows():
        sems = (ag_s, ag_r)

        def same(i, j, rows, n, device):
            return remote(h_all.at[i, j, rows], h_all.at[i, j, rows], sems, n, device)

        full = pl.ds(0, 64)
        started = [same(x, core, lo, 0, to_p), same(x, core, hi, 1, to_m), same(x, core, full, 2, to_c),
                   same(x, core, hi, 3, to_p), same(x, core, lo, 4, to_m)]
        for copy in started:
            copy.start()
        pump.turn()
        settle()

        def go(copy):
            copy.start()
            started.append(copy)

        pump.idle(7.0)
        same(xm, core, lo, 0, to_p).wait_recv()
        go(same(xm, core, lo, 5, to_p))
        go(same(xm, core, lo, 7, to_c))
        same(xp, core, hi, 1, to_p).wait_recv()
        go(same(xp, core, hi, 6, to_m))
        go(same(xp, core, hi, 8, to_c))
        pump.idle(4.0)
        same(xm, core, hi, 3, to_p).wait_recv()
        go(same(xm, core, hi, 9, to_c))
        same(xp, core, lo, 4, to_p).wait_recv()
        go(same(xp, core, lo, 10, to_c))
        pump.idle(4.0)
        same(x2, core, lo, 5, to_p).wait_recv()
        go(same(x2, core, lo, 11, to_c))
        same(x2, core, hi, 6, to_p).wait_recv()
        go(same(x2, core, hi, 12, to_c))
        pump.idle(2.0)
        for i, rows, n in ((x, full, 2), (xm, lo, 7), (xp, hi, 8), (xm, hi, 9), (xp, lo, 10), (x2, lo, 11), (x2, hi, 12)):
            same(i, other, rows, n, to_p).wait_recv()
        leaving.extend(started)

    def add_rows(product, cross_us, src_ref, dst_ref):
        sems = (rs_s, rs_r)
        sent = []

        def go(copy):
            copy.start()
            sent.append(copy)

        def cols_of(c):
            return pl.ds(c * CHUNK, CHUNK)

        def cross(c):
            return remote(part.at[:, other, :, cols_of(c)], cx.at[:, :, cols_of(c)], sems, 7 * c, to_c)

        def first(c, side):
            n, rows, to = ((1, lo, to_p), (2, hi, to_m))[side]
            return remote(part.at[x2, core, rows, cols_of(c)], rx1.at[side, :, cols_of(c)], sems, 7 * c + n, to)

        def second(c, side, late):
            n = 3 + 2 * side + late
            rows = (hi, lo)[side ^ late]
            blk, to = ((xp, to_p), (xm, to_m))[side]
            return remote(part.at[blk, core, rows, cols_of(c)], rx2.at[side, rows, cols_of(c)], sems, 7 * c + n, to)

        def stage_b(c):
            cross(c).wait_recv()
            cols = cols_of(c)
            for i in range(NX):
                part[i, core, :, cols] = part[i, core, :, cols] + cx[i, :, cols]
            for side in (0, 1):
                go(first(c, side))
            for side in (0, 1):
                go(second(c, side, 0))

        def stage_c(c):
            cols = cols_of(c)
            for side in (0, 1):
                first(c, side).wait_recv()
                blk, rows = ((xp, lo), (xm, hi))[side]
                part[blk, core, rows, cols] = part[blk, core, rows, cols] + rx1[side, :, cols]
                go(second(c, side, 1))

        def stage_d(c):
            cols = cols_of(c)
            for side in (0, 1):
                for late in (0, 1):
                    second(c, side, late).wait_recv()
            total = part[x, core, :, cols] + rx2[0, :, cols] + rx2[1, :, cols]
            dst_ref[:, cols] = (src_ref[:, cols].astype(F32) + total).astype(BF16)

        for c in range(NCH):
            product(c)
            go(cross(c))
            if c >= 1:
                pump.idle(cross_us)
                stage_b(c - 1)
            if c >= 2:
                stage_c(c - 2)
        pump.idle(1.0)
        settle()
        pump.idle(1.5)
        stage_b(NCH - 1)
        pump.idle(4.5)
        stage_c(NCH - 2)
        pump.idle(4.5)
        stage_c(NCH - 1)
        for c in range(NCH):
            pump.idle((0.3, 1.5, 3.0, 3.0)[c])
            stage_d(c)
        leaving.extend(sent)

    rows_q = lax.broadcasted_iota(jnp.int32, (64, 64), 0)
    cols_k = lax.broadcasted_iota(jnp.int32, (64, 64), 1)
    one_head = (rows_q >= cols_k).astype(F32)
    seen = jnp.concatenate([one_head] * 3, axis=0) > 0.5

    def attend(wref):
        for first, width in ((0, 256), (256, 256), (512, 128)):
            pump.fill(1.0)
            h = h_all[...].reshape(512, D)
            w = wref[:, :, :, first:first + width].reshape(D, width)
            acc = jnp.dot(h, w, preferred_element_type=F32)
            part[:, :, :, first:first + width] = acc.astype(BF16).astype(F32).reshape(4, 2, 64, width)
            pump.work(1.0)

        def pair(i, carry):
            c2, n2 = cos2[...], sin2[...]
            c3, n3 = jnp.concatenate([c2] * 3, axis=0), jnp.concatenate([n2] * 3, axis=0)

            def turn(v, c, n):
                return (v * c + pltpu.roll(v, HD // 2, 1) * n).astype(BF16)

            both = []
            for j in range(2):
                rows = pl.ds(pl.multiple_of(i * 16 + j * 8, 8), 8)
                heads = [part[:, :, rows, h * HD:(h + 1) * HD].reshape(64, HD) for h in range(5)]
                both.append((rows, jnp.concatenate(heads[:3], axis=0), heads[3], heads[4]))
            outs = []
            for rows, q, k, v in both:
                sc = lax.dot_general(turn(q, c3, n3), turn(k, c2, n2), (((1,), (1,)), ((), ())),
                                     preferred_element_type=F32) * SCALE
                sc = jnp.where(seen, sc, -jnp.inf)
                e = jnp.exp(sc - jnp.max(sc, axis=-1, keepdims=True))
                p = (e / jnp.sum(e, axis=-1, keepdims=True)).astype(BF16)
                outs.append(jnp.dot(p, v.astype(BF16), preferred_element_type=F32).astype(BF16).astype(F32))
            for (rows, _, _, _), o in zip(both, outs):
                for h in range(3):
                    part[:, :, rows, h * HD:(h + 1) * HD] = o[h * 64:(h + 1) * 64].reshape(4, 2, 8, HD)
            return carry

        for half in range(2):
            pump.fill(ATTEND_US)
            lax.fori_loop(half * 2, half * 2 + 2, pair, 0)
            pump.work(ATTEND_US)
        zbuf[:, 0:384] = part[:, :, :, 0:384].reshape(512, 384).astype(BF16)

    def out_product(wref, first, width, us):
        def product(c):
            def plane(i, carry):
                zi = 2 * c + i
                w = wref[zi, :, :, first:first + width].reshape(4 * ROWS, width)
                acc = lax.dot_general(zbuf[:, 0:width], w, (((1,), (1,)), ((), ())), preferred_element_type=F32)
                cols = pl.ds(pl.multiple_of(zi * 384, 128), 384)
                part[:, :, :, cols] = acc.reshape(4, 2, 64, 384)
                return carry

            pump.fill(us)
            lax.fori_loop(0, 2, plane, 0)
            pump.work(us)
        return product

    def mlp_hidden(wref):
        def tile(i, carry):
            h = h_all[...].reshape(512, D)
            c0 = pl.multiple_of(1024 + i * 256, 256)
            c1 = pl.multiple_of(2048 + i * 256, 256)
            g = jnp.dot(h, wref[:, :, :, pl.ds(c0, 256)].reshape(D, 256), preferred_element_type=F32)
            u = jnp.dot(h, wref[:, :, :, pl.ds(c1, 256)].reshape(D, 256), preferred_element_type=F32)
            zbuf[:, pl.ds(pl.multiple_of(i * 256, 256), 256)] = (jax.nn.silu(g) * u).astype(BF16)
            return carry

        for half in range(2):
            pump.fill(3.7)
            lax.fori_loop(half * 2, half * 2 + 2, tile, 0)
            pump.work(3.7)

    for layer, wref in ((0, w0), (1, w1)):
        src = x_ref if layer == 0 else res
        if layer:
            norm(src, gain_a, layer)
            pump.work(1.0)
        gather_rows()
        pump.group(3 * layer)
        attend(wref)
        add_rows(out_product(wref, 640, 384, 0.7), 1.8, src, res)
        norm(res, gain_m, layer)
        pump.work(1.0)
        gather_rows()
        pump.group(3 * layer + 1)
        mlp_hidden(wref)
        pump.group(3 * layer + 2)
        down = out_product(w0, 3072, 1024, 1.5)
        if layer == 0:
            add_rows(down, 1.0, res, res)
        else:
            pump.sent(2)
            copies = [pltpu.make_async_copy(wlast.at[2 * c:2 * c + 2], w0.at[2 * c:2 * c + 2, :, :, 3072:4096], csem.at[c])
                      for c in range(NCH)]
            for copy in copies:
                copy.start()

            def last(c):
                copies[c].wait()
                down(c)

            add_rows(last, 1.0, res, y_ref)
    settle()
    pump.finish()


def solution(mesh):
    act_spec = P('fsdp', 'model', None)
    col_spec = P(None, 'fsdp', 'model')
    row_spec = P(None, 'model', 'fsdp')

    def device_step(x_in, gain_attn, gain_mlp, rope_cos, rope_sin, w_q, w_k, w_v, w_o, w_gate, w_up, w_down):
        wo_t = jnp.swapaxes(w_o, 1, 2)
        wd_t = jnp.swapaxes(w_down, 1, 2)
        vmem = pl.BlockSpec(memory_space=pltpu.VMEM)
        hbm = pl.BlockSpec(memory_space=pltpu.HBM)
        n_slabs = len(SLABS)
        out, _ = pl.pallas_call(
            kernel,
            name="layers",
            out_shape=(jax.ShapeDtypeStruct((64, D), BF16), jax.ShapeDtypeStruct((NZ, NY, ROWS, 1024), BF16)),
            in_specs=[vmem] * 5 + [hbm] * 7,
            out_specs=(vmem, hbm),
            scratch_shapes=[
                pltpu.VMEM((NZ, NY, ROWS, 4096), BF16),
                pltpu.VMEM((NZ, NY, ROWS, 3072), BF16),
                pltpu.VMEM((4, 2, 64, D), BF16),
                pltpu.VMEM((4, 2, 64, D), F32),
                pltpu.VMEM((4, 64, D), F32),
                pltpu.VMEM((2, 32, D), F32),
                pltpu.VMEM((2, 64, D), F32),
                pltpu.VMEM((512, 1024), BF16),
                pltpu.VMEM((64, D), BF16),
                pltpu.VMEM((ROWS, 1024), BF16),
                pltpu.VMEM((64, HD), F32),
                pltpu.VMEM((64, HD), F32),
                pltpu.SemaphoreType.DMA((16,)),
                pltpu.SemaphoreType.DMA((NCH,)),
                pltpu.SemaphoreType.DMA((n_slabs,)),
                pltpu.SemaphoreType.DMA((n_slabs, 10)),
                pltpu.SemaphoreType.DMA((13,)),
                pltpu.SemaphoreType.DMA((13,)),
                pltpu.SemaphoreType.DMA((7 * NCH,)),
                pltpu.SemaphoreType.DMA((7 * NCH,)),
            ],
            compiler_params=pltpu.CompilerParams(
                collective_id=0, has_side_effects=True, vmem_limit_bytes=67043328),
        )(x_in.reshape(64, D), gain_attn, gain_mlp, rope_cos, rope_sin, w_q, w_k, w_v, wo_t, w_gate, w_up, wd_t)
        return out.reshape(x_in.shape)

    return jax.shard_map(device_step, mesh=mesh, in_specs=(act_spec, P(), P(), P(), P(), col_spec, col_spec, col_spec, row_spec, col_spec, col_spec, row_spec), out_specs=act_spec, check_vma=False)
```

```python
import heapq

import jax
import jax.numpy as jnp
from jax import lax
from jax.experimental import pallas as pl
from jax.experimental.pallas import tpu as pltpu
from jax.sharding import PartitionSpec as P

EPS = 1e-5
MESH = pl.DeviceIdType.MESH
NZ, NY, NX = 8, 4, 4
D = 3072
HD = 128
ROWS = 96
CHUNK = 768
NCH = D // CHUNK
SCALE = HD ** -0.5
F32, BF16 = jnp.float32, jnp.bfloat16

GROUPS = (
    (0, 0, (2, 2, 2, 2)),
    (0, 1024, (3, 1, 6, 6)),
    (0, 3072, (2, 2, 2, 2)),
    (1, 0, (1, 2, 3, 2)),
    (1, 1024, (5, 5, 3, 3)),
    (1, 3072, (1, 2, 2, 3)),
)
WEIGHT = (-99.0, -94.5, -56.5, -43.0, 35.0, 35.0)
OFFSET = {"A": (-50.0, 47.0), "B": (-16.0, 14.5)}
SIGN = 1
AHEAD, MARGIN = 2.5, 1.5
ATTEND_US = 2.3
RATE, LAT = 46.3e3, 2.2
SEND_US, RECEIVE_US = 0.06, 0.04


def make_slabs(groups):
    slabs = []
    for g, (layer, first, tiles) in enumerate(groups):
        col = first
        for kind, dirn, n in zip("AABB", (1, -1, 1, -1), tiles):
            if n:
                slabs.append(dict(g=g, layer=layer, c0=col, n=n * 128, kind=kind, dirn=dirn))
            col += n * 128
    return slabs


def hop(slab, t):
    if slab["kind"] == "A":
        return ("y", t, 1) if t < 3 else ("z", t - 3, 4)
    return ("z", t, 1) if t < 7 else ("y", t - 7, 8)


class Planner:
    def __init__(self, slabs, weight, offset, sign, ahead, margin):
        self.slabs, self.weight, self.offset, self.sign, self.ahead, self.margin = slabs, weight, offset, sign, ahead, margin
        self.spent = 0.0
        self.links = [(ax, d) for ax in "yz" for d in (1, -1)]
        self.busy = {k: 0.0 for k in self.links}
        self.ready = {k: [] for k in self.links}
        self.heap, self.clock = [], 0.0
        self.due = {}
        self.ends = {}
        for i, slab in enumerate(slabs):
            self.ready[(hop(slab, 0)[0], slab["dirn"])].append((i, 0))
            self.due[slab["g"]] = self.due.get(slab["g"], 0) + 10

    def rank(self, item):
        slab, t = self.slabs[item[0]], item[1]
        late = 0 if t < (3 if slab["kind"] == "A" else 7) else 1
        return (self.weight[slab["g"]] + self.offset[slab["kind"]][late], self.sign * t, item)

    def send(self, i, t):
        pass

    def receive(self, i, t):
        pass

    def turn(self):
        while self.heap and self.heap[0][0] <= self.clock:
            _, i, t = heapq.heappop(self.heap)
            self.receive(i, t)
            self.spent += RECEIVE_US
            g = self.slabs[i]["g"]
            self.due[g] -= 1
            self.ends[g] = self.clock
            if t < 9:
                self.ready[(hop(self.slabs[i], t + 1)[0], self.slabs[i]["dirn"])].append((i, t + 1))
        self.issue(self.ahead)

    def issue(self, ahead):
        for k in self.links:
            while self.ready[k] and self.busy[k] - self.clock < ahead:
                item = min(self.ready[k], key=self.rank)
                self.ready[k].remove(item)
                i, t = item
                size = hop(self.slabs[i], t)[2] * ROWS * self.slabs[i]["n"] * 2
                self.busy[k] = max(self.clock, self.busy[k]) + size / RATE
                self.send(i, t)
                self.spent += SEND_US
                heapq.heappush(self.heap, (self.busy[k] + LAT, i, t))

    def fill(self, us):
        self.spent = 0.0
        self.issue(us + self.margin)
        self.clock += self.spent

    def work(self, us):
        self.clock += us
        self.spent = 0.0
        self.turn()
        self.clock += self.spent

    def idle(self, us):
        end = self.clock + us
        while self.heap and self.heap[0][0] <= end:
            self.clock = max(self.clock, self.heap[0][0])
            self.turn()
        self.clock = end

    def group(self, g):
        while self.due[g]:
            self.clock = max(self.clock, self.heap[0][0])
            self.turn()


SLABS = make_slabs(GROUPS)


class Pump(Planner):
    def __init__(self, place, where, before, spare, ssem, rsem):
        super().__init__(SLABS, WEIGHT, OFFSET, SIGN, AHEAD, MARGIN)
        z, y, self.m = place
        self.z, self.y = z, y
        self.where, self.before, self.spare, self.ssem, self.rsem = where, before, spare, ssem, rsem
        self.left = set(range(len(SLABS)))
        self.zs = [z] + [lax.rem(z + u, NZ) for u in range(1, NZ)]
        self.ys = [y] + [lax.rem(y + u, NY) for u in range(1, NY)]
        self.to = {("y", d): z * NY + self.ys[d % NY] for d in (1, -1)}
        self.to.update({("z", d): self.zs[d % NZ] * NY + y for d in (1, -1)})

    def desc(self, i, t):
        slab = SLABS[i]
        d = slab["dirn"]
        axis, u, blocks = hop(slab, t)
        ref, base = self.where(slab)
        cols = pl.ds(slab["c0"] - base, slab["n"])
        if axis == "y":
            yi = self.ys[-d * u % NY]
            part = ref.at[self.z, yi, :, cols] if blocks == 1 else ref.at[:, yi, :, cols]
        else:
            zi = self.zs[-d * u % NZ]
            part = ref.at[zi, self.y, :, cols] if blocks == 1 else ref.at[zi, :, :, cols]
        return pltpu.make_async_remote_copy(
            src_ref=part, dst_ref=part, send_sem=self.ssem.at[i], recv_sem=self.rsem.at[i, t],
            device_id=(self.to[axis, d], self.m), device_id_type=MESH)

    def send(self, i, t):
        if t == 0:
            self.before(SLABS[i])
        self.desc(i, t).start()

    def receive(self, i, t):
        self.desc(i, t).wait_recv()

    def sent(self, g):
        self.group(g)
        for i in sorted(i for i in self.left if SLABS[i]["g"] == g):
            whole = self.spare.at[pl.ds(0, NZ * NY - 1), :, pl.ds(0, SLABS[i]["n"])]
            pltpu.make_async_copy(whole, whole, self.ssem.at[i]).wait()
            self.left.remove(i)

    def finish(self):
        for g in range(len(GROUPS)):
            self.sent(g)


def kernel(x_ref, gain_a, gain_m, cos_ref, sin_ref, wq, wk, wv, wo, wg, wu, wd,
           y_ref, wlast, w0, w1, h_all, part, cx, rx1, rx2, zbuf, res, stage, cos2, sin2,
           lsem, csem, ssem, rsem, ag_s, ag_r, rs_s, rs_r):
    f = lax.axis_index("fsdp")
    m = lax.axis_index("model")
    z, y = f // NY, lax.rem(f, NY)
    x, core = m // 2, lax.rem(m, 2)
    xp, xm, x2 = lax.rem(x + 1, NX), lax.rem(x + 3, NX), lax.rem(x + 2, NX)
    other = 1 - core
    to_p, to_m, to_c = (f, xp * 2 + core), (f, xm * 2 + core), (f, x * 2 + other)

    loads = []
    for layer, ref in ((0, w0), (1, w1)):
        col = 0
        for src, width in ((wq, 384), (wk, 128), (wv, 128), (wo, 384), (wg, 1024), (wu, 1024), (wd, 1024)):
            to = ref.at[z, y, :, pl.ds(col, width)] if col + width <= ref.shape[-1] else stage
            copy = pltpu.make_async_copy(src.at[layer], to, lsem.at[len(loads)])
            copy.start()
            loads.append((layer, col, width, copy))
            col += width
    waited = set()

    def before(slab):
        for n, (layer, col, width, copy) in enumerate(loads):
            if layer == slab["layer"] and col < slab["c0"] + slab["n"] and slab["c0"] < col + width and n not in waited:
                waited.add(n)
                if n < len(loads) - 1:
                    copy.wait()

    bar = pltpu.get_barrier_semaphore()
    partners = [to_p, to_m, to_c]
    partners += [(z * NY + lax.rem(y + d, NY), m) for d in (1, NY - 1)]
    partners += [(lax.rem(z + d, NZ) * NY + y, m) for d in (1, NZ - 1)]
    for device in partners:
        pl.semaphore_signal(bar, inc=1, device_id=device, device_id_type=MESH)

    def norm(src_ref, gain_ref, layer):
        total = jnp.zeros((64, 1), F32)
        for c in range(NCH):
            v = src_ref[:, c * CHUNK:(c + 1) * CHUNK].astype(F32)
            total += jnp.sum(v * v, axis=-1, keepdims=True)
        inv = lax.rsqrt(total * (1.0 / D) + EPS)
        for c in range(NCH):
            cols = slice(c * CHUNK, (c + 1) * CHUNK)
            v = src_ref[:, cols].astype(F32)
            h_all[x, core, :, cols] = (v * inv * gain_ref[layer:layer + 1, cols]).astype(BF16)

    norm(x_ref, gain_a, 0)
    cos2[...] = jnp.concatenate([cos_ref[...], cos_ref[...]], axis=-1)
    sin2[...] = jnp.concatenate([-sin_ref[...], sin_ref[...]], axis=-1)

    loads[-1][3].wait()
    out = pltpu.make_async_copy(stage, wlast.at[z, y], lsem.at[len(loads)])
    out.start()
    pl.semaphore_wait(bar, len(partners))
    out.wait()

    def where(slab):
        if slab["layer"] == 0:
            return w0, 0
        return (w1, 0) if slab["c0"] < 3072 else (wlast, 3072)

    pump = Pump((z, y, m), where, before, wlast.reshape(NZ * NY, ROWS, 1024), ssem, rsem)

    def remote(src, dst, sems, n, device):
        return pltpu.make_async_remote_copy(
            src_ref=src, dst_ref=dst, send_sem=sems[0].at[n], recv_sem=sems[1].at[n],
            device_id=device, device_id_type=MESH)

    lo, hi = pl.ds(0, 32), pl.ds(32, 32)
    leaving = []

    def settle():
        for copy in leaving:
            copy.wait_send()
        leaving.clear()

    def gather_rows():
        sems = (ag_s, ag_r)

        def same(i, j, rows, n, device):
            return remote(h_all.at[i, j, rows], h_all.at[i, j, rows], sems, n, device)

        full = pl.ds(0, 64)
        started = [same(x, core, lo, 0, to_p), same(x, core, hi, 1, to_m), same(x, core, full, 2, to_c),
                   same(x, core, hi, 3, to_p), same(x, core, lo, 4, to_m)]
        for copy in started:
            copy.start()
        pump.turn()
        settle()

        def go(copy):
            copy.start()
            started.append(copy)

        pump.idle(7.0)
        same(xm, core, lo, 0, to_p).wait_recv()
        go(same(xm, core, lo, 5, to_p))
        go(same(xm, core, lo, 7, to_c))
        same(xp, core, hi, 1, to_p).wait_recv()
        go(same(xp, core, hi, 6, to_m))
        go(same(xp, core, hi, 8, to_c))
        pump.idle(4.0)
        same(xm, core, hi, 3, to_p).wait_recv()
        go(same(xm, core, hi, 9, to_c))
        same(xp, core, lo, 4, to_p).wait_recv()
        go(same(xp, core, lo, 10, to_c))
        pump.idle(4.0)
        same(x2, core, lo, 5, to_p).wait_recv()
        go(same(x2, core, lo, 11, to_c))
        same(x2, core, hi, 6, to_p).wait_recv()
        go(same(x2, core, hi, 12, to_c))
        pump.idle(2.0)
        for i, rows, n in ((x, full, 2), (xm, lo, 7), (xp, hi, 8), (xm, hi, 9), (xp, lo, 10), (x2, lo, 11), (x2, hi, 12)):
            same(i, other, rows, n, to_p).wait_recv()
        leaving.extend(started)

    def add_rows(product, cross_us, src_ref, dst_ref, last=False):
        sems = (rs_s, rs_r)
        sent = []

        def go(copy):
            copy.start()
            sent.append(copy)

        def cols_of(c):
            return pl.ds(c * CHUNK, CHUNK)

        def cross(c):
            return remote(part.at[:, other, :, cols_of(c)], cx.at[:, :, cols_of(c)], sems, 7 * c, to_c)

        def first(c, side):
            n, rows, to = ((1, lo, to_p), (2, hi, to_m))[side]
            return remote(part.at[x2, core, rows, cols_of(c)], rx1.at[side, :, cols_of(c)], sems, 7 * c + n, to)

        def second(c, side, late):
            n = 3 + 2 * side + late
            rows = (hi, lo)[side ^ late]
            blk, to = ((xp, to_p), (xm, to_m))[side]
            return remote(part.at[blk, core, rows, cols_of(c)], rx2.at[side, rows, cols_of(c)], sems, 7 * c + n, to)

        def stage_b(c):
            cross(c).wait_recv()
            cols = cols_of(c)
            for i in range(NX):
                part[i, core, :, cols] = part[i, core, :, cols] + cx[i, :, cols]
            for side in (0, 1):
                go(first(c, side))
            for side in (0, 1):
                go(second(c, side, 0))

        def stage_c(c):
            cols = cols_of(c)
            for side in (0, 1):
                first(c, side).wait_recv()
                blk, rows = ((xp, lo), (xm, hi))[side]
                part[blk, core, rows, cols] = part[blk, core, rows, cols] + rx1[side, :, cols]
                go(second(c, side, 1))

        def stage_d(c):
            cols = cols_of(c)
            for side in (0, 1):
                for late in (0, 1):
                    second(c, side, late).wait_recv()
            total = part[x, core, :, cols] + rx2[0, :, cols] + rx2[1, :, cols]
            dst_ref[:, cols] = (src_ref[:, cols].astype(F32) + total).astype(BF16)

        for c in range(NCH):
            product(c)
            go(cross(c))
            if c >= 1:
                pump.idle(cross_us)
                stage_b(c - 1)
            if c >= 2:
                stage_c(c - 2)
        pump.idle(1.0)
        settle()
        pump.idle(1.5)
        stage_b(NCH - 1)
        pump.idle(4.5)
        stage_c(NCH - 2)
        pump.idle(4.5)
        stage_c(NCH - 1)
        for c in range(NCH):
            pump.idle((0.3, 1.5, 3.0, 3.0)[c])
            if last and c == NCH - 1:
                pump.finish()
                for copy in sent:
                    copy.wait_send()
                sent.clear()
            stage_d(c)
        leaving.extend(sent)

    rows_q = lax.broadcasted_iota(jnp.int32, (64, 64), 0)
    cols_k = lax.broadcasted_iota(jnp.int32, (64, 64), 1)
    one_head = (rows_q >= cols_k).astype(F32)
    seen = jnp.concatenate([one_head] * 3, axis=0) > 0.5

    def attend(wref):
        for first, width in ((0, 256), (256, 256), (512, 128)):
            pump.fill(1.0)
            h = h_all[...].reshape(512, D)
            w = wref[:, :, :, first:first + width].reshape(D, width)
            acc = jnp.dot(h, w, preferred_element_type=F32)
            part[:, :, :, first:first + width] = acc.astype(BF16).astype(F32).reshape(4, 2, 64, width)
            pump.work(1.0)

        def pair(i, carry):
            c2, n2 = cos2[...], sin2[...]
            c3, n3 = jnp.concatenate([c2] * 3, axis=0), jnp.concatenate([n2] * 3, axis=0)

            def turn(v, c, n):
                return (v * c + pltpu.roll(v, HD // 2, 1) * n).astype(BF16)

            both = []
            for j in range(2):
                rows = pl.ds(pl.multiple_of(i * 16 + j * 8, 8), 8)
                heads = [part[:, :, rows, h * HD:(h + 1) * HD].reshape(64, HD) for h in range(5)]
                both.append((rows, jnp.concatenate(heads[:3], axis=0), heads[3], heads[4]))
            outs = []
            for rows, q, k, v in both:
                sc = lax.dot_general(turn(q, c3, n3), turn(k, c2, n2), (((1,), (1,)), ((), ())),
                                     preferred_element_type=F32) * SCALE
                sc = jnp.where(seen, sc, -jnp.inf)
                e = jnp.exp(sc - jnp.max(sc, axis=-1, keepdims=True))
                p = (e / jnp.sum(e, axis=-1, keepdims=True)).astype(BF16)
                outs.append(jnp.dot(p, v.astype(BF16), preferred_element_type=F32).astype(BF16).astype(F32))
            for (rows, _, _, _), o in zip(both, outs):
                for h in range(3):
                    part[:, :, rows, h * HD:(h + 1) * HD] = o[h * 64:(h + 1) * 64].reshape(4, 2, 8, HD)
            return carry

        for half in range(2):
            pump.fill(ATTEND_US)
            lax.fori_loop(half * 2, half * 2 + 2, pair, 0)
            pump.work(ATTEND_US)
        zbuf[:, 0:384] = part[:, :, :, 0:384].reshape(512, 384).astype(BF16)

    def out_product(wref, first, width, us):
        def product(c):
            def plane(i, carry):
                zi = 2 * c + i
                w = wref[zi, :, :, first:first + width].reshape(4 * ROWS, width)
                acc = lax.dot_general(zbuf[:, 0:width], w, (((1,), (1,)), ((), ())), preferred_element_type=F32)
                cols = pl.ds(pl.multiple_of(zi * 384, 128), 384)
                part[:, :, :, cols] = acc.reshape(4, 2, 64, 384)
                return carry

            pump.fill(us)
            lax.fori_loop(0, 2, plane, 0)
            pump.work(us)
        return product

    def mlp_hidden(wref):
        def tile(i, carry):
            h = h_all[...].reshape(512, D)
            c0 = pl.multiple_of(1024 + i * 256, 256)
            c1 = pl.multiple_of(2048 + i * 256, 256)
            g = jnp.dot(h, wref[:, :, :, pl.ds(c0, 256)].reshape(D, 256), preferred_element_type=F32)
            u = jnp.dot(h, wref[:, :, :, pl.ds(c1, 256)].reshape(D, 256), preferred_element_type=F32)
            zbuf[:, pl.ds(pl.multiple_of(i * 256, 256), 256)] = (jax.nn.silu(g) * u).astype(BF16)
            return carry

        for half in range(2):
            pump.fill(3.7)
            lax.fori_loop(half * 2, half * 2 + 2, tile, 0)
            pump.work(3.7)

    for layer, wref in ((0, w0), (1, w1)):
        src = x_ref if layer == 0 else res
        if layer:
            norm(src, gain_a, layer)
            pump.work(1.0)
        gather_rows()
        pump.group(3 * layer)
        attend(wref)
        add_rows(out_product(wref, 640, 384, 0.7), 1.8, src, res)
        norm(res, gain_m, layer)
        pump.work(1.0)
        gather_rows()
        pump.group(3 * layer + 1)
        mlp_hidden(wref)
        pump.group(3 * layer + 2)
        down = out_product(w0, 3072, 1024, 1.5)
        if layer == 0:
            add_rows(down, 1.0, res, res)
        else:
            pump.sent(2)
            copies = [pltpu.make_async_copy(wlast.at[2 * c:2 * c + 2], w0.at[2 * c:2 * c + 2, :, :, 3072:4096], csem.at[c])
                      for c in range(NCH)]
            for copy in copies:
                copy.start()

            def final(c):
                copies[c].wait()
                down(c)

            add_rows(final, 1.0, res, y_ref, last=True)


def solution(mesh):
    act_spec = P('fsdp', 'model', None)
    col_spec = P(None, 'fsdp', 'model')
    row_spec = P(None, 'model', 'fsdp')

    def device_step(x_in, gain_attn, gain_mlp, rope_cos, rope_sin, w_q, w_k, w_v, w_o, w_gate, w_up, w_down):
        wo_t = jnp.swapaxes(w_o, 1, 2)
        wd_t = jnp.swapaxes(w_down, 1, 2)
        vmem = pl.BlockSpec(memory_space=pltpu.VMEM)
        hbm = pl.BlockSpec(memory_space=pltpu.HBM)
        n_slabs = len(SLABS)
        out, _ = pl.pallas_call(
            kernel,
            name="layers",
            out_shape=(jax.ShapeDtypeStruct((64, D), BF16), jax.ShapeDtypeStruct((NZ, NY, ROWS, 1024), BF16)),
            in_specs=[vmem] * 5 + [hbm] * 7,
            out_specs=(vmem, hbm),
            scratch_shapes=[
                pltpu.VMEM((NZ, NY, ROWS, 4096), BF16),
                pltpu.VMEM((NZ, NY, ROWS, 3072), BF16),
                pltpu.VMEM((4, 2, 64, D), BF16),
                pltpu.VMEM((4, 2, 64, D), F32),
                pltpu.VMEM((4, 64, D), F32),
                pltpu.VMEM((2, 32, D), F32),
                pltpu.VMEM((2, 64, D), F32),
                pltpu.VMEM((512, 1024), BF16),
                pltpu.VMEM((64, D), BF16),
                pltpu.VMEM((ROWS, 1024), BF16),
                pltpu.VMEM((64, HD), F32),
                pltpu.VMEM((64, HD), F32),
                pltpu.SemaphoreType.DMA((16,)),
                pltpu.SemaphoreType.DMA((NCH,)),
                pltpu.SemaphoreType.DMA((n_slabs,)),
                pltpu.SemaphoreType.DMA((n_slabs, 10)),
                pltpu.SemaphoreType.DMA((13,)),
                pltpu.SemaphoreType.DMA((13,)),
                pltpu.SemaphoreType.DMA((7 * NCH,)),
                pltpu.SemaphoreType.DMA((7 * NCH,)),
            ],
            compiler_params=pltpu.CompilerParams(
                collective_id=0, has_side_effects=True, vmem_limit_bytes=67043328),
        )(x_in.reshape(64, D), gain_attn, gain_mlp, rope_cos, rope_sin, w_q, w_k, w_v, wo_t, w_gate, w_up, wd_t)
        return out.reshape(x_in.shape)

    return jax.shard_map(device_step, mesh=mesh, in_specs=(act_spec, P(), P(), P(), P(), col_spec, col_spec, col_spec, row_spec, col_spec, col_spec, row_spec), out_specs=act_spec, check_vma=False)
```
